32 devices in a mesh: dp: 4 (over z), tensor: 8 (over y, x, core).
Axes of the slice: x: 2, y: 2, z: 4, core: 2. Of those that a mesh axis runs over, the one named last changes fastest.
Arguments:
- projected: bfloat16 [2, 4096, 4608], P(None, ('dp', 'tensor')), may hold values from -60 to 60
- out_grad: bfloat16 [2, 4096, 4608], P(None, ('dp', 'tensor')), may hold values from -20 to 20
- attention: bfloat16 [2, 4096, 4096], P(None, 'dp', 'tensor'), may hold values from -6 to 6
- w_out: bfloat16 [4096, 4608], P('tensor'), may hold values from -0.09375 to 0.09375
- gains: float32 [4608], replicated, may hold values from 0.5 to 1.5
- main_out: float32 [4096, 4608], P('tensor', 'dp'), may hold values from -6 to 6
- main_gains: float32 [4608], replicated, may hold values from -6 to 6
Outputs:
- attn_grad: bfloat16 [2, 4096, 4096], P(None, 'dp', 'tensor')
- new_main_out: float32 [4096, 4608], P('tensor', 'dp')
- new_main_gains: float32 [4608], replicated
The draws below stay inside these ranges and needn't reach their ends.
All inputs are finite; a program needn't handle non-finite values.
Results may differ from the reference program's by a relative error of at most 0.0049.
Values may be sent and summed in bfloat16 or wider, within the bound.
A program may use at most 128 MiB of HBM per device.

```python
import math
import jax
import jax.numpy as jnp
from jax import lax

D = 4608
HQ = 4096
MICRO = 2
ROWS = 4096


def spread_values(key, shape):
    first, second, third = jax.random.split(key, 3)
    base = jnp.clip(jax.random.normal(first, shape), -6.0, 6.0)
    columns = jnp.exp(jax.random.uniform(second, (shape[-1],), minval=math.log(0.3), maxval=math.log(3.0)))
    row_scale = jnp.exp(jax.random.uniform(third, shape[:-1] + (1,), minval=math.log(0.3), maxval=math.log(3.0)))
    return base * row_scale * columns


def rising_values(key, shape):
    position = jnp.arange(shape[1], dtype=jnp.float32) / shape[1]
    base = jnp.clip(jax.random.normal(key, shape), -6.0, 6.0)
    growth = jnp.exp(position * math.log(3.0))
    return base * growth[None, :, None]


def draw_projected(key, part):
    return spread_values(jax.random.fold_in(key, 22), (MICRO, ROWS, D)).astype(jnp.bfloat16)


def draw_out_grad(key, part):
    return rising_values(jax.random.fold_in(key, 33), (MICRO, ROWS, D)).astype(jnp.bfloat16)


def steps_of(stream_key, dims, cuts, low, high):
    def one(axis_at, shards_of):
        steps = jax.random.uniform(jax.random.fold_in(jax.random.fold_in(stream_key, 6), axis_at), (shards_of,), jnp.float32, low / len(cuts), high / len(cuts))
        return jnp.repeat(jnp.exp(steps), dims[axis_at] // shards_of).reshape((-1,) + (1,) * (len(dims) - axis_at - 1))

    loudness = one(*cuts[0])
    for cut in cuts[1:]:
        loudness = loudness * one(*cut)
    return loudness


def scatter_about(own_key, dims, spread, reach, cuts=(), held_as=jnp.bfloat16):
    result = jax.random.normal(own_key, dims, jnp.float32) * spread
    if len(cuts) > 0:
        result = steps_of(own_key, dims, cuts, -0.22, 0.18) * result
    return jnp.clip(result, min=-reach, max=reach).astype(held_as)


def setup_inputs(seed: int = 0) -> dict:
    keys = jax.random.split(jax.random.key(seed), 8)
    return {
        "projected": draw_projected(jax.random.fold_in(keys[7], 71), 0),
        "out_grad": draw_out_grad(jax.random.fold_in(keys[7], 71), 0),
        "attention": scatter_about(keys[2], (MICRO, ROWS, HQ), 1.0, 6.0, ((1, 4), (2, 8))),
        "w_out": scatter_about(keys[3], (HQ, D), HQ ** -0.5, 0.09375, ((0, 8),)),
        "gains": jnp.clip(1.0 + 0.1 * jax.random.normal(keys[4], (D,), jnp.float32), 0.5, 1.5),
        "main_out": scatter_about(keys[5], (HQ, D), 1.0, 6.0, ((0, 8), (1, 4)), jnp.float32),
        "main_gains": scatter_about(keys[6], (D,), 1.0, 6.0, (), jnp.float32),
    }


def normalized(values):
    inverse = lax.rsqrt(lax.optimization_barrier(jnp.mean(values * values, axis=-1, keepdims=True)) + 1e-06)
    return (values * inverse, inverse)

def norm_back(upstream, normed, inverse):
    return inverse * (upstream - normed * lax.optimization_barrier(jnp.mean(upstream * normed, axis=-1, keepdims=True)))

def reference(projected, out_grad, attention, w_out, gains, main_out, main_gains):
    factor = 1.0 / (MICRO * ROWS) ** 0.5
    sum_out = jnp.zeros((HQ, D), jnp.float32)
    sum_gain = jnp.zeros((D,), jnp.float32)
    attn_list = []
    for micro_step in range(MICRO):
        output_in = projected[micro_step].astype(jnp.float32)
        upstream = out_grad[micro_step].astype(jnp.float32)
        out_hat, out_inv = normalized(output_in)
        out_gain = lax.optimization_barrier(jnp.sum(upstream * out_hat, axis=0))
        out_back = norm_back(upstream * gains, out_hat, out_inv).astype(jnp.bfloat16)
        attn_list.append(jnp.dot(out_back, w_out.T, preferred_element_type=jnp.float32).astype(jnp.bfloat16))
        sum_out = sum_out + jnp.dot(attention[micro_step].T, out_back, preferred_element_type=jnp.float32)
        sum_gain = sum_gain + out_gain
    return (jnp.stack(attn_list), main_out + factor * sum_out, main_gains + factor * sum_gain)
```

```python
import functools
import math

import jax
import jax.numpy as jnp
from jax import lax
from jax.experimental import pallas as pl
from jax.experimental.pallas import tpu as pltpu
from jax.sharding import PartitionSpec as P

MESH = pl.DeviceIdType.MESH
LANES = 128
TILE = 16


def flip(index, step):
    return index + step * (1 - 2 * (lax.div(index, step) % 2))


def combine(index, steps):
    found = [index]
    for step in steps:
        found = found + [flip(each, step) for each in found]
    return found


def kernel(
    dims,
    proj_hbm, grad_hbm, att_hbm, w_hbm, gains_ref,
    attn_hbm, sum_hbm, gain_hbm,
    own_in, held, w_buf, att_in, att_t, acc, part, arrived, out_sum, gain_acc, gain_mine, gain_got,
    in_sem, w_sem, att_sem, out_sem,
    ag_send, ag_recv, pair_send, pair_recv, rs_send, rs_recv, gain_send, gain_recv,
):
    T, DP, D_true, micro, own, heads, wide, K = dims
    w = LANES
    R = micro * own
    L = (T // 2).bit_length() - 1
    C = T // 2
    t_me = lax.axis_index("tensor")
    d_me = lax.axis_index("dp")
    d_width = wide // DP
    t_pair = flip(t_me, 1)
    chip_steps = [2 << bit for bit in range(L)]
    cuts = [R * i // L // TILE * TILE for i in range(L)] + [R]

    blocks = 8
    height = R // blocks

    def load(block):
        slot = block % 2
        rows = pl.ds(block * height, height)
        return (
            pltpu.make_async_copy(proj_hbm.at[rows], own_in.at[slot, 0], in_sem.at[slot, 0]),
            pltpu.make_async_copy(grad_hbm.at[rows], own_in.at[slot, 1], in_sem.at[slot, 1]),
        )

    for block in range(2):
        for copy in load(block):
            copy.start()

    def att_load(t, slot):
        return [
            pltpu.make_async_copy(
                att_hbm.at[m, pl.ds(t * own, own)], att_in.at[slot, pl.ds(m * own, own)], att_sem.at[slot, m]
            )
            for m in range(micro)
        ]

    for t in range(2):
        for copy in att_load(t, t):
            copy.start()

    def w_load(k, d):
        return pltpu.make_async_copy(
            w_hbm.at[:, pl.ds(pl.multiple_of(d * d_width + k * w, w), w)],
            w_buf.at[k, :, pl.ds(d * w, w)],
            w_sem.at[k, d],
        )

    barrier = pltpu.get_barrier_semaphore()
    partners = [("tensor", t_pair)] + [("tensor", flip(t_me, step)) for step in chip_steps]
    dp_steps = [1 << bit for bit in range(DP.bit_length() - 1)]
    partners += [("dp", flip(d_me, step)) for step in dp_steps]
    for name, where in partners:
        pl.semaphore_signal(barrier, inc=1, device_id={name: where}, device_id_type=MESH)

    @pl.when(d_me > 0)
    def _():
        pl.semaphore_signal(barrier, inc=1, device_id={"dp": d_me - 1}, device_id_type=MESH)

    @pl.when(d_me < DP - 1)
    def _():
        pl.semaphore_signal(barrier, inc=1, device_id={"dp": d_me + 1}, device_id_type=MESH)

    gain_acc[...] = jnp.zeros_like(gain_acc)
    own_base = pl.multiple_of(t_me * R, R)
    for block in range(blocks):
        slot = block % 2
        for copy in load(block):
            copy.wait()

        def rows_step(i, carry, slot=slot, block=block):
            rows = pl.ds(pl.multiple_of(i * TILE, TILE), TILE)
            v = own_in[slot, 0, rows, :].astype(jnp.float32)
            g = own_in[slot, 1, rows, :].astype(jnp.float32)
            u = g * gains_ref[...]
            r = lax.rsqrt(jnp.sum(v * v, axis=-1, keepdims=True) * (1.0 / D_true) + 1e-6)
            n = v * r
            m = jnp.sum(u * n, axis=-1, keepdims=True) * (1.0 / D_true)
            gn = g * n
            gain_acc[...] += gn[:8] + gn[8:]
            back = (r * (u - n * m)).astype(jnp.bfloat16)
            at = pl.ds(pl.multiple_of(own_base + block * height + i * TILE, TILE), TILE)
            for k in range(K):
                for d in range(DP):
                    c0 = d * d_width + k * w
                    held[k, at, d * w:(d + 1) * w] = back[:, c0:c0 + w]
            return carry

        lax.fori_loop(0, height // TILE, rows_step, 0)
        if block + 2 < blocks:
            for copy in load(block + 2):
                copy.start()
    gain_mine[0] = jnp.sum(gain_acc[...], axis=0, keepdims=True)

    waits = len(partners) + jnp.where(d_me > 0, 1, 0) + jnp.where(d_me < DP - 1, 1, 0)
    pl.semaphore_wait(barrier, waits)

    def block_of(k, t, p):
        if p is None:
            return held.at[k, pl.ds(pl.multiple_of(t * R, R), R)]
        return held.at[k, pl.ds(pl.multiple_of(t * R + cuts[p], TILE), cuts[p + 1] - cuts[p])]

    def stage_copies(k, s, receive):
        copies = []
        for p in range(L):
            bits = [chip_steps[(p + i) % L] for i in range(s + 1)]
            peer = flip(t_me, bits[s])
            first = peer if receive else t_me
            for j, src in enumerate(combine(first, bits[:s])):
                index = p * (C - 1) + (1 << s) - 1 + j
                ref = block_of(k, src, p)
                copies.append((p, index, src, pltpu.make_async_remote_copy(
                    src_ref=ref, dst_ref=ref, send_sem=ag_send.at[k, index], recv_sem=ag_recv.at[k, index],
                    device_id={"tensor": peer}, device_id_type=MESH)))
        return copies

    def pair_copy(k, index, src, p):
        ref = block_of(k, src, p)
        return pltpu.make_async_remote_copy(
            src_ref=ref, dst_ref=ref, send_sem=pair_send.at[k, index], recv_sem=pair_recv.at[k, index],
            device_id={"tensor": t_pair}, device_id_type=MESH)

    own_index = L * (C - 1)

    def advance(k, s):
        if s > 0:
            for p, index, src, copy in stage_copies(k, s - 1, True):
                copy.wait_recv()
                if s == L:
                    pair_copy(k, index, src, p).start()
        if s < L:
            for _, _, _, copy in stage_copies(k, s, False):
                copy.start()
            if s > 0:
                for p, index, src, _ in stage_copies(k, s - 1, True):
                    pair_copy(k, index, src, p).start()
            else:
                pair_copy(k, own_index, t_me, None).start()

    def all_received_from_pair(k):
        for s in range(L):
            for p, index, src, _ in stage_copies(k, s, True):
                pair_copy(k, index, flip(src, 1), p).wait_recv()
        pair_copy(k, own_index, t_pair, None).wait_recv()

    def all_sent(k):
        for s in range(L):
            for _, _, _, copy in stage_copies(k, s, False):
                copy.wait_send()
            for p, index, src, _ in stage_copies(k, s, True):
                pair_copy(k, index, src, p).wait_send()
        pair_copy(k, own_index, t_me, None).wait_send()

    def start_w(k, carry):
        for d in range(DP):
            w_load(k, d).start()
        return carry

    def rs_copy(k, d, to_left):
        if to_left:
            slot = jnp.where(d_me - 1 == d, DP, d)
            peer = d_me - 1
        else:
            slot, peer = d, d_me + 1
        return pltpu.make_async_remote_copy(
            src_ref=arrived.at[k, d], dst_ref=arrived.at[k, slot], send_sem=rs_send.at[k, d],
            recv_sem=rs_recv.at[k, slot], device_id={"dp": peer}, device_id_type=MESH)

    def rs_arrival(k, slot):
        return pltpu.make_async_remote_copy(
            src_ref=arrived.at[k, slot], dst_ref=arrived.at[k, slot], send_sem=rs_send.at[k, 0],
            recv_sem=rs_recv.at[k, slot], device_id={"dp": flip(d_me, 1)}, device_id_type=MESH)

    gain_steps = [("tensor", 1)] + [("tensor", s) for s in chip_steps] + [("dp", s) for s in dp_steps]
    S = len(gain_steps)

    def gain_copy(s):
        name, step = gain_steps[s]
        return pltpu.make_async_remote_copy(
            src_ref=gain_mine.at[s], dst_ref=gain_got.at[s], send_sem=gain_send.at[s], recv_sem=gain_recv.at[s],
            device_id={name: flip(t_me if name == "tensor" else d_me, step)}, device_id_type=MESH)

    def within(k):
        return jnp.logical_and(k >= 0, k < K)

    for q in range(min(L, K)):
        advance(q, 0)
    lax.fori_loop(0, K, start_w, 0)

    def turn(t, carry):
        slot = t % 2
        for copy in att_load(t, slot):
            copy.wait()
        att_t[:, pl.ds(pl.multiple_of(t * R, R), R)] = att_in[slot].astype(jnp.float32).T.astype(jnp.bfloat16)

        @pl.when(t + 2 < T)
        def _():
            for copy in att_load(t + 2, slot):
                copy.start()
        return carry

    lax.fori_loop(0, T, turn, 0)

    big = 2 * R
    tiles = T * R // big

    def step(i, carry):
        c = i - (L - 1)
        for s in range(L + 1):
            q = c + L - s

            @pl.when(jnp.logical_and(within(q), jnp.logical_or(q >= L, s > 0)))
            def _(q=q, s=s):
                advance(q, s)

        @pl.when(within(c))
        def _():
            all_received_from_pair(c)
            part[c % DP] = jnp.dot(att_t[...], held[c], preferred_element_type=jnp.float32)

        right = c - d_me
        left = c - (DP - 1 - d_me)
        final = jnp.minimum(left, right)

        def pass_on(k, d, to_left, has_arrival):
            piece = part[k % DP, :, d * w:(d + 1) * w]

            @pl.when(has_arrival)
            def _():
                rs_arrival(k, d).wait_recv()
                arrived[k, d] = (piece + arrived[k, d].astype(jnp.float32)).astype(jnp.bfloat16)

            @pl.when(jnp.logical_not(has_arrival))
            def _():
                arrived[k, d] = piece.astype(jnp.bfloat16)

            rs_copy(k, d, to_left).start()

        for d in reversed(range(1, DP)):
            @pl.when(jnp.logical_and(within(right), d_me < d))
            def _(d=d):
                pass_on(right, d, False, d_me > 0)
        for d in range(DP - 1):
            @pl.when(jnp.logical_and(within(left), d_me > d))
            def _(d=d):
                pass_on(left, d, True, d_me < DP - 1)

        @pl.when(within(c))
        def _():
            for d in range(DP):
                w_load(c, d).wait()

            def tile(n, carry):
                rows = pl.ds(pl.multiple_of(n * big, big), big)
                product = lax.dot_general(
                    held[c, rows, :], w_buf[c], (((1,), (1,)), ((), ())), preferred_element_type=jnp.float32)

                @pl.when(c == 0)
                def _():
                    acc[rows, :] = product

                @pl.when(c > 0)
                def _():
                    acc[rows, :] += product
                return carry

            lax.fori_loop(0, tiles, tile, 0)
            all_sent(c)

        @pl.when(c == K - 1)
        def _():
            def leave(t, carry):
                rows = pl.ds(pl.multiple_of(t * R, R), R)
                held[0, rows, :heads] = acc[rows, :].astype(jnp.bfloat16)
                for m in range(micro):
                    attn_copy(t, m).start()
                return carry
            lax.fori_loop(0, T, leave, 0)

        @pl.when(within(final))
        def _():
            mine = part[final % DP, :, pl.ds(pl.multiple_of(d_me * w, w), w)]
            at = pl.ds(pl.multiple_of(final * w, w), w)
            out_sum[:, at] = mine

            @pl.when(d_me > 0)
            def _():
                rs_arrival(final, d_me).wait_recv()
                out_sum[:, at] += arrived[final, d_me].astype(jnp.float32)

            @pl.when(d_me < DP - 1)
            def _():
                rs_arrival(final, DP).wait_recv()
                out_sum[:, at] += arrived[final, DP].astype(jnp.float32)

        for s in range(S + 1):
            @pl.when(c == s)
            def _(s=s):
                if s > 0:
                    gain_copy(s - 1).wait()
                    gain_mine[s] = gain_mine[s - 1] + gain_got[s - 1]
                if s < S:
                    gain_copy(s).start()
        return carry

    def attn_copy(t, m):
        return pltpu.make_async_copy(
            held.at[0, pl.ds(pl.multiple_of(t * R + m * own, TILE), own), pl.ds(0, heads)],
            attn_hbm.at[m, pl.ds(pl.multiple_of(t * own, TILE), own)],
            out_sem.at[t, m],
        )

    total = max(K + DP - 1, S + 1)
    lax.fori_loop(0, total + L - 1, step, 0)

    sum_out = pltpu.make_async_copy(out_sum, sum_hbm, in_sem.at[0, 0])
    gain_out = pltpu.make_async_copy(gain_mine.at[S], gain_hbm, in_sem.at[0, 1])
    sum_out.start()
    gain_out.start()

    def drain(k, carry):
        for d in range(DP):
            @pl.when(d != d_me)
            def _(d=d):
                pltpu.make_async_remote_copy(
                    src_ref=arrived.at[k, d], dst_ref=arrived.at[k, d], send_sem=rs_send.at[k, d],
                    recv_sem=rs_recv.at[k, d], device_id={"dp": flip(d_me, 1)}, device_id_type=MESH).wait_send()
        return carry

    lax.fori_loop(0, K, drain, 0)

    def attn_wait(t, carry):
        for m in range(micro):
            attn_copy(t, m).wait()
        return carry

    lax.fori_loop(0, T, attn_wait, 0)
    sum_out.wait()
    gain_out.wait()


def padded(values, parts, axis):
    size = values.shape[axis] // parts
    extra = -size % LANES
    if extra == 0:
        return values
    shape = values.shape
    split = values.reshape(shape[:axis] + (parts, size) + shape[axis + 1:])
    pads = [(0, 0)] * split.ndim
    pads[axis + 1] = (0, extra)
    return jnp.pad(split, pads).reshape(shape[:axis] + (parts * (size + extra),) + shape[axis + 1:])


def unpadded(values, parts, size, axis):
    have = values.shape[axis] // parts
    if have == size:
        return values
    shape = values.shape
    split = values.reshape(shape[:axis] + (parts, have) + shape[axis + 1:])
    split = lax.slice_in_dim(split, 0, size, axis=axis + 1)
    return split.reshape(shape[:axis] + (parts * size,) + shape[axis + 1:])


def per_device(projected, out_grad, attention, w_out, gains, main_out, main_gains):
    T, DP = lax.axis_size("tensor"), lax.axis_size("dp")
    micro, own, D = projected.shape
    heads = w_out.shape[0]
    piece = D // DP
    factor = 1.0 / math.sqrt(micro * own * DP * T)
    R = micro * own
    proj = padded(projected.reshape(R, D), DP, 1)
    grad = padded(out_grad.reshape(R, D), DP, 1)
    weight = padded(w_out, DP, 1)
    gain_row = padded(gains.reshape(1, D), DP, 1)
    wide = proj.shape[1]
    K = wide // DP // LANES
    C = T // 2
    L = C.bit_length() - 1
    S = 1 + L + DP.bit_length() - 1
    chunk = DP * LANES
    dims = (T, DP, D, micro, own, heads, wide, K)
    count = L * (C - 1)
    DMA = pltpu.SemaphoreType.DMA
    anywhere = pl.BlockSpec(memory_space=pl.ANY)
    attn_grad, total, gain_total = pl.pallas_call(
        functools.partial(kernel, dims),
        out_shape=(
            jax.ShapeDtypeStruct((micro, own * T, heads), jnp.bfloat16),
            jax.ShapeDtypeStruct((heads, wide // DP), jnp.float32),
            jax.ShapeDtypeStruct((1, wide), jnp.float32),
        ),
        in_specs=[anywhere] * 4 + [pl.BlockSpec(memory_space=pltpu.VMEM)],
        out_specs=(anywhere,) * 3,
        scratch_shapes=[
            pltpu.VMEM((2, 2, R // 8, wide), jnp.bfloat16),
            pltpu.VMEM((K, T * R, chunk), jnp.bfloat16),
            pltpu.VMEM((K, heads, chunk), jnp.bfloat16),
            pltpu.VMEM((2, R, heads), jnp.bfloat16),
            pltpu.VMEM((heads, T * R), jnp.bfloat16),
            pltpu.VMEM((T * R, heads), jnp.float32),
            pltpu.VMEM((DP, heads, chunk), jnp.float32),
            pltpu.VMEM((K, DP + 1, heads, LANES), jnp.bfloat16),
            pltpu.VMEM((heads, wide // DP), jnp.float32),
            pltpu.VMEM((8, wide), jnp.float32),
            pltpu.VMEM((S + 1, 1, wide), jnp.float32),
            pltpu.VMEM((S, 1, wide), jnp.float32),
            DMA((2, 2)), DMA((K, DP)), DMA((2, micro)), DMA((T, micro)),
            DMA((K, count)), DMA((K, count)), DMA((K, count + 1)), DMA((K, count + 1)),
            DMA((K, DP)), DMA((K, DP + 1)), DMA((S,)), DMA((S,)),
        ],
        compiler_params=pltpu.CompilerParams(
            collective_id=0, has_side_effects=True, vmem_limit_bytes=67043328
        ),
    )(proj, grad, attention, weight, gain_row)
    total = unpadded(total, 1, piece, 1)
    gain_total = unpadded(gain_total, DP, piece, 1).reshape(D)
    return (attn_grad, main_out + factor * total, main_gains + factor * gain_total)


def solution(mesh):
    placed = (
        P(None, ("dp", "tensor"), None),
        P(None, ("dp", "tensor"), None),
        P(None, "dp", "tensor"),
        P("tensor", None),
        P(),
        P("tensor", "dp"),
        P(),
    )
    return jax.shard_map(
        per_device,
        mesh=mesh,
        in_specs=placed,
        out_specs=(P(None, "dp", "tensor"), P("tensor", "dp"), P()),
        check_vma=False,
    )
```

```python
import functools
import math

import jax
import jax.numpy as jnp
from jax import lax
from jax.experimental import pallas as pl
from jax.experimental.pallas import tpu as pltpu
from jax.sharding import PartitionSpec as P

MESH = pl.DeviceIdType.MESH
LANES = 128
TILE = 16


def flip(index, step):
    return index + step * (1 - 2 * (lax.div(index, step) % 2))


def combine(index, steps):
    found = [index]
    for step in steps:
        found = found + [flip(each, step) for each in found]
    return found


def kernel(
    dims,
    factor,
    proj_hbm, grad_hbm, att_hbm, w_hbm, main_hbm, gains_ref,
    attn_hbm, sum_hbm, gain_hbm,
    own_in, held, w_buf, att_in, att_t, acc, part, arrived, out_sum, gain_acc, gain_mine, gain_got,
    in_sem, w_sem, att_sem, out_sem, main_sem,
    ag_send, ag_recv, pair_send, pair_recv, rs_send, rs_recv, gain_send, gain_recv,
):
    T, DP, D_true, micro, own, heads, wide, K = dims
    w = LANES
    R = micro * own
    L = (T // 2).bit_length() - 1
    C = T // 2
    t_me = lax.axis_index("tensor")
    d_me = lax.axis_index("dp")
    d_width = wide // DP
    t_pair = flip(t_me, 1)
    chip_steps = [2 << bit for bit in range(L)]
    cuts = [R * i // L // TILE * TILE for i in range(L)] + [R]

    blocks = 8
    height = R // blocks

    def load(block):
        slot = block % 2
        rows = pl.ds(block * height, height)
        return (
            pltpu.make_async_copy(proj_hbm.at[rows], own_in.at[slot, 0], in_sem.at[slot, 0]),
            pltpu.make_async_copy(grad_hbm.at[rows], own_in.at[slot, 1], in_sem.at[slot, 1]),
        )

    for block in range(2):
        for copy in load(block):
            copy.start()

    def att_load(t, slot):
        return [
            pltpu.make_async_copy(
                att_hbm.at[m, pl.ds(t * own, own)], att_in.at[slot, pl.ds(m * own, own)], att_sem.at[slot, m]
            )
            for m in range(micro)
        ]

    for t in range(2):
        for copy in att_load(t, t):
            copy.start()
    main_in = pltpu.make_async_copy(main_hbm, out_sum, main_sem)

    def w_load(k, d):
        return pltpu.make_async_copy(
            w_hbm.at[:, pl.ds(pl.multiple_of(d * d_width + k * w, w), w)],
            w_buf.at[k, :, pl.ds(d * w, w)],
            w_sem.at[k, d],
        )

    barrier = pltpu.get_barrier_semaphore()
    partners = [("tensor", t_pair)] + [("tensor", flip(t_me, step)) for step in chip_steps]
    dp_steps = [1 << bit for bit in range(DP.bit_length() - 1)]
    partners += [("dp", flip(d_me, step)) for step in dp_steps]
    for name, where in partners:
        pl.semaphore_signal(barrier, inc=1, device_id={name: where}, device_id_type=MESH)

    @pl.when(d_me > 0)
    def _():
        pl.semaphore_signal(barrier, inc=1, device_id={"dp": d_me - 1}, device_id_type=MESH)

    @pl.when(d_me < DP - 1)
    def _():
        pl.semaphore_signal(barrier, inc=1, device_id={"dp": d_me + 1}, device_id_type=MESH)

    gain_acc[...] = jnp.zeros_like(gain_acc)
    own_base = pl.multiple_of(t_me * R, R)
    for block in range(blocks):
        slot = block % 2
        for copy in load(block):
            copy.wait()

        def rows_step(i, carry, slot=slot, block=block):
            rows = pl.ds(pl.multiple_of(i * TILE, TILE), TILE)
            v = own_in[slot, 0, rows, :].astype(jnp.float32)
            g = own_in[slot, 1, rows, :].astype(jnp.float32)
            u = g * gains_ref[...].reshape(1, wide)
            r = lax.rsqrt(jnp.sum(v * v, axis=-1, keepdims=True) * (1.0 / D_true) + 1e-6)
            n = v * r
            m = jnp.sum(u * n, axis=-1, keepdims=True) * (1.0 / D_true)
            gn = g * n
            gain_acc[...] += gn[:8] + gn[8:]
            back = (r * (u - n * m)).astype(jnp.bfloat16)
            at = pl.ds(pl.multiple_of(own_base + block * height + i * TILE, TILE), TILE)
            for k in range(K):
                for d in range(DP):
                    c0 = d * d_width + k * w
                    held[k, at, d * w:(d + 1) * w] = back[:, c0:c0 + w]
            return carry

        lax.fori_loop(0, height // TILE, rows_step, 0)
        if block + 2 < blocks:
            for copy in load(block + 2):
                copy.start()
    gain_mine[0] = jnp.sum(gain_acc[...], axis=0, keepdims=True)

    waits = len(partners) + jnp.where(d_me > 0, 1, 0) + jnp.where(d_me < DP - 1, 1, 0)
    pl.semaphore_wait(barrier, waits)

    def block_of(k, t, p):
        if p is None:
            return held.at[k, pl.ds(pl.multiple_of(t * R, R), R)]
        return held.at[k, pl.ds(pl.multiple_of(t * R + cuts[p], TILE), cuts[p + 1] - cuts[p])]

    def stage_copies(k, s, receive):
        copies = []
        for p in range(L):
            bits = [chip_steps[(p + i) % L] for i in range(s + 1)]
            peer = flip(t_me, bits[s])
            first = peer if receive else t_me
            for j, src in enumerate(combine(first, bits[:s])):
                index = p * (C - 1) + (1 << s) - 1 + j
                ref = block_of(k, src, p)
                copies.append((p, index, src, pltpu.make_async_remote_copy(
                    src_ref=ref, dst_ref=ref, send_sem=ag_send.at[k, index], recv_sem=ag_recv.at[k, index],
                    device_id={"tensor": peer}, device_id_type=MESH)))
        return copies

    def pair_copy(k, index, src, p):
        ref = block_of(k, src, p)
        return pltpu.make_async_remote_copy(
            src_ref=ref, dst_ref=ref, send_sem=pair_send.at[k, index], recv_sem=pair_recv.at[k, index],
            device_id={"tensor": t_pair}, device_id_type=MESH)

    own_index = L * (C - 1)

    def advance(k, s):
        if s > 0:
            for p, index, src, copy in stage_copies(k, s - 1, True):
                copy.wait_recv()
                if s == L:
                    pair_copy(k, index, src, p).start()
        if s < L:
            for _, _, _, copy in stage_copies(k, s, False):
                copy.start()
            if s > 0:
                for p, index, src, _ in stage_copies(k, s - 1, True):
                    pair_copy(k, index, src, p).start()
            else:
                pair_copy(k, own_index, t_me, None).start()

    def all_received_from_pair(k):
        for s in range(L):
            for p, index, src, _ in stage_copies(k, s, True):
                pair_copy(k, index, flip(src, 1), p).wait_recv()
        pair_copy(k, own_index, t_pair, None).wait_recv()

    def all_sent(k):
        for s in range(L):
            for _, _, _, copy in stage_copies(k, s, False):
                copy.wait_send()
            for p, index, src, _ in stage_copies(k, s, True):
                pair_copy(k, index, src, p).wait_send()
        pair_copy(k, own_index, t_me, None).wait_send()

    def start_w(k, carry):
        for d in range(DP):
            w_load(k, d).start()
        return carry

    def rs_copy(k, d, to_left):
        if to_left:
            slot = jnp.where(d_me - 1 == d, DP, d)
            peer = d_me - 1
        else:
            slot, peer = d, d_me + 1
        return pltpu.make_async_remote_copy(
            src_ref=arrived.at[k, d], dst_ref=arrived.at[k, slot], send_sem=rs_send.at[k, d],
            recv_sem=rs_recv.at[k, slot], device_id={"dp": peer}, device_id_type=MESH)

    def rs_arrival(k, slot):
        return pltpu.make_async_remote_copy(
            src_ref=arrived.at[k, slot], dst_ref=arrived.at[k, slot], send_sem=rs_send.at[k, 0],
            recv_sem=rs_recv.at[k, slot], device_id={"dp": flip(d_me, 1)}, device_id_type=MESH)

    gain_steps = [("tensor", 1)] + [("tensor", s) for s in chip_steps] + [("dp", s) for s in dp_steps]
    S = len(gain_steps)

    def gain_copy(s):
        name, step = gain_steps[s]
        return pltpu.make_async_remote_copy(
            src_ref=gain_mine.at[s], dst_ref=gain_got.at[s], send_sem=gain_send.at[s], recv_sem=gain_recv.at[s],
            device_id={name: flip(t_me if name == "tensor" else d_me, step)}, device_id_type=MESH)

    def within(k):
        return jnp.logical_and(k >= 0, k < K)

    for q in range(min(L, K)):
        advance(q, 0)
    lax.fori_loop(0, K, start_w, 0)
    main_in.start()

    def turn(t, carry):
        slot = t % 2
        for copy in att_load(t, slot):
            copy.wait()
        att_t[:, pl.ds(pl.multiple_of(t * R, R), R)] = att_in[slot].astype(jnp.float32).T.astype(jnp.bfloat16)

        @pl.when(t + 2 < T)
        def _():
            for copy in att_load(t + 2, slot):
                copy.start()
        return carry

    lax.fori_loop(0, T // 2, turn, 0)
    advance(0, 1)
    lax.fori_loop(T // 2, T, turn, 0)
    main_in.wait()

    big = 2 * R
    tiles = T * R // big

    def step(i, carry):
        c = i - (L - 1)
        for s in range(L + 1):
            q = c + L - s

            @pl.when(jnp.logical_and(within(q), q >= (L if s == 0 else 1 if s == 1 else 0)))
            def _(q=q, s=s):
                advance(q, s)

        @pl.when(within(c))
        def _():
            all_received_from_pair(c)
            part[c % DP] = jnp.dot(att_t[...], held[c], preferred_element_type=jnp.float32)

        right = c - d_me
        left = c - (DP - 1 - d_me)
        final = jnp.minimum(left, right)

        def pass_on(k, d, to_left, has_arrival):
            piece = part[k % DP, :, d * w:(d + 1) * w]

            @pl.when(has_arrival)
            def _():
                rs_arrival(k, d).wait_recv()
                arrived[k, d] = (piece + arrived[k, d].astype(jnp.float32)).astype(jnp.bfloat16)

            @pl.when(jnp.logical_not(has_arrival))
            def _():
                arrived[k, d] = piece.astype(jnp.bfloat16)

            rs_copy(k, d, to_left).start()

        for d in reversed(range(1, DP)):
            @pl.when(jnp.logical_and(within(right), d_me < d))
            def _(d=d):
                pass_on(right, d, False, d_me > 0)
        for d in range(DP - 1):
            @pl.when(jnp.logical_and(within(left), d_me > d))
            def _(d=d):
                pass_on(left, d, True, d_me < DP - 1)

        @pl.when(within(c))
        def _():
            for d in range(DP):
                w_load(c, d).wait()

            def tile(n, carry):
                rows = pl.ds(pl.multiple_of(n * big, big), big)
                product = lax.dot_general(
                    held[c, rows, :], w_buf[c], (((1,), (1,)), ((), ())), preferred_element_type=jnp.float32)

                @pl.when(c == 0)
                def _():
                    acc[rows, :] = product

                @pl.when(c > 0)
                def _():
                    acc[rows, :] += product
                return carry

            lax.fori_loop(0, tiles, tile, 0)
            all_sent(c)

        @pl.when(c == K - 1)
        def _():
            def leave(t, carry):
                rows = pl.ds(pl.multiple_of(t * R, R), R)
                held[0, rows, :heads] = acc[rows, :].astype(jnp.bfloat16)
                for m in range(micro):
                    attn_copy(t, m).start()
                return carry
            lax.fori_loop(0, T, leave, 0)

        @pl.when(within(final))
        def _():
            mine = part[final % DP, :, pl.ds(pl.multiple_of(d_me * w, w), w)]
            at = pl.ds(pl.multiple_of(final * w, w), w)
            out_sum[:, at] += factor * mine

            @pl.when(d_me > 0)
            def _():
                rs_arrival(final, d_me).wait_recv()
                out_sum[:, at] += factor * arrived[final, d_me].astype(jnp.float32)

            @pl.when(d_me < DP - 1)
            def _():
                rs_arrival(final, DP).wait_recv()
                out_sum[:, at] += factor * arrived[final, DP].astype(jnp.float32)

        for s in range(S + 1):
            @pl.when(c == s)
            def _(s=s):
                if s > 0:
                    gain_copy(s - 1).wait()
                    gain_mine[s] = gain_mine[s - 1] + gain_got[s - 1]
                if s < S:
                    gain_copy(s).start()
        return carry

    def attn_copy(t, m):
        return pltpu.make_async_copy(
            held.at[0, pl.ds(pl.multiple_of(t * R + m * own, TILE), own), pl.ds(0, heads)],
            attn_hbm.at[m, pl.ds(pl.multiple_of(t * own, TILE), own)],
            out_sem.at[t, m],
        )

    total = max(K + DP - 1, S + 1)
    lax.fori_loop(0, total + L - 1, step, 0)

    sum_out = pltpu.make_async_copy(out_sum, sum_hbm, in_sem.at[0, 0])
    gain_out = pltpu.make_async_copy(gain_mine.at[S], gain_hbm, in_sem.at[0, 1])
    sum_out.start()
    gain_out.start()

    def drain(k, carry):
        for d in range(DP):
            @pl.when(d != d_me)
            def _(d=d):
                pltpu.make_async_remote_copy(
                    src_ref=arrived.at[k, d], dst_ref=arrived.at[k, d], send_sem=rs_send.at[k, d],
                    recv_sem=rs_recv.at[k, d], device_id={"dp": flip(d_me, 1)}, device_id_type=MESH).wait_send()
        return carry

    lax.fori_loop(0, K, drain, 0)

    def attn_wait(t, carry):
        for m in range(micro):
            attn_copy(t, m).wait()
        return carry

    lax.fori_loop(0, T, attn_wait, 0)
    sum_out.wait()
    gain_out.wait()


def padded(values, parts, axis):
    size = values.shape[axis] // parts
    extra = -size % LANES
    if extra == 0:
        return values
    shape = values.shape
    split = values.reshape(shape[:axis] + (parts, size) + shape[axis + 1:])
    pads = [(0, 0)] * split.ndim
    pads[axis + 1] = (0, extra)
    return jnp.pad(split, pads).reshape(shape[:axis] + (parts * (size + extra),) + shape[axis + 1:])


def unpadded(values, parts, size, axis):
    have = values.shape[axis] // parts
    if have == size:
        return values
    shape = values.shape
    split = values.reshape(shape[:axis] + (parts, have) + shape[axis + 1:])
    split = lax.slice_in_dim(split, 0, size, axis=axis + 1)
    return split.reshape(shape[:axis] + (parts * size,) + shape[axis + 1:])


def per_device(projected, out_grad, attention, w_out, gains, main_out, main_gains):
    T, DP = lax.axis_size("tensor"), lax.axis_size("dp")
    micro, own, D = projected.shape
    heads = w_out.shape[0]
    piece = D // DP
    factor = 1.0 / math.sqrt(micro * own * DP * T)
    R = micro * own
    proj = padded(projected.reshape(R, D), DP, 1)
    grad = padded(out_grad.reshape(R, D), DP, 1)
    weight = padded(w_out, DP, 1)
    gain_row = padded(gains, DP, 0)
    main = padded(main_out, 1, 1)
    wide = proj.shape[1]
    K = wide // DP // LANES
    C = T // 2
    L = C.bit_length() - 1
    S = 1 + L + DP.bit_length() - 1
    chunk = DP * LANES
    dims = (T, DP, D, micro, own, heads, wide, K)
    count = L * (C - 1)
    DMA = pltpu.SemaphoreType.DMA
    anywhere = pl.BlockSpec(memory_space=pl.ANY)
    attn_grad, total, gain_total = pl.pallas_call(
        functools.partial(kernel, dims, factor),
        out_shape=(
            jax.ShapeDtypeStruct((micro, own * T, heads), jnp.bfloat16),
            jax.ShapeDtypeStruct((heads, wide // DP), jnp.float32),
            jax.ShapeDtypeStruct((1, wide), jnp.float32),
        ),
        in_specs=[anywhere] * 5 + [pl.BlockSpec(memory_space=pltpu.VMEM)],
        out_specs=(anywhere,) * 3,
        scratch_shapes=[
            pltpu.VMEM((2, 2, R // 8, wide), jnp.bfloat16),
            pltpu.VMEM((K, T * R, chunk), jnp.bfloat16),
            pltpu.VMEM((K, heads, chunk), jnp.bfloat16),
            pltpu.VMEM((2, R, heads), jnp.bfloat16),
            pltpu.VMEM((heads, T * R), jnp.bfloat16),
            pltpu.VMEM((T * R, heads), jnp.float32),
            pltpu.VMEM((DP, heads, chunk), jnp.float32),
            pltpu.VMEM((K, DP + 1, heads, LANES), jnp.bfloat16),
            pltpu.VMEM((heads, wide // DP), jnp.float32),
            pltpu.VMEM((8, wide), jnp.float32),
            pltpu.VMEM((S + 1, 1, wide), jnp.float32),
            pltpu.VMEM((S, 1, wide), jnp.float32),
            DMA((2, 2)), DMA((K, DP)), DMA((2, micro)), DMA((T, micro)), DMA,
            DMA((K, count)), DMA((K, count)), DMA((K, count + 1)), DMA((K, count + 1)),
            DMA((K, DP)), DMA((K, DP + 1)), DMA((S,)), DMA((S,)),
        ],
        compiler_params=pltpu.CompilerParams(
            collective_id=0, has_side_effects=True, vmem_limit_bytes=67043328
        ),
    )(proj, grad, attention, weight, main, gain_row)
    total = unpadded(total, 1, piece, 1)
    gain_total = unpadded(gain_total, DP, piece, 1).reshape(D)
    return (attn_grad, total, main_gains + factor * gain_total)


def solution(mesh):
    placed = (
        P(None, ("dp", "tensor"), None),
        P(None, ("dp", "tensor"), None),
        P(None, "dp", "tensor"),
        P("tensor", None),
        P(),
        P("tensor", "dp"),
        P(),
    )
    return jax.shard_map(
        per_device,
        mesh=mesh,
        in_specs=placed,
        out_specs=(P(None, "dp", "tensor"), P("tensor", "dp"), P()),
        check_vma=False,
    )
```
